512 devices in a mesh: dp: 8 (over x, core), expert: 64 (over z, y).
Axes of the slice: x: 4, y: 8, z: 8, core: 2. Of those that a mesh axis runs over, the one named last changes fastest.
Arguments:
- tokens: bfloat16 [65536, 2048], P(('dp', 'expert')), may hold values from -160 to 160
- router_weight: bfloat16 [2048, 64], replicated, may hold values from -0.25 to 0.25
- route_ids: int32 [65536, 2], P(('dp', 'expert')), may hold values from 0 to 63, as said below
- gate_weight: bfloat16 [64, 768, 2048], P('expert', 'dp'), may hold values from -0.125 to 0.125
- up_weight: bfloat16 [64, 768, 2048], P('expert', 'dp'), may hold values from -0.125 to 0.125
- down_weight: bfloat16 [64, 768, 2048], P('expert', 'dp'), may hold values from -0.21875 to 0.21875
Outputs:
- mixture: bfloat16 [65536, 2048], P(('dp', 'expert'))
- z_loss: float32 [], replicated
The draws below stay inside these ranges and needn't reach their ends.
Inputs may be any that keep to these rules, and one draw needn't show every extreme that they name: `route_ids`: each row names 2 different experts; among the rows of one device no expert is named more than 5 times, and one expert is named exactly 5 times by the rows of every device.
All inputs are finite; a program needn't handle non-finite values.
Results may differ from the reference program's by a relative error of at most 0.0057.
Values may be sent and summed in bfloat16 or wider, within the bound.
A program may use at most 64 MiB of HBM per device.

```python
import math
import jax
import jax.numpy as jnp
from jax import lax

D = 2048
FF = 768
EXP_DEV = 1
TOPK = 2
TOK_DEV = 128
EXPERTS = 64
CAP = 5
TOKENS = 65536


def router_table(key):
    base_key = jax.random.fold_in(key, 7)
    bound_value = math.sqrt(3.0 / D)
    values = jax.random.uniform(base_key, (D, EXPERTS), jnp.float32, -bound_value, bound_value)
    return values.astype(jnp.bfloat16).astype(jnp.float32)


def expert_order(subkey):
    return jax.random.permutation(subkey, EXPERTS)


def token_order(subkey):
    return jax.random.permutation(subkey, TOK_DEV)


def route_table(key):
    blocks = TOKENS // TOK_DEV
    slots_dev = TOK_DEV * TOPK
    base_count = slots_dev // EXPERTS
    spare = CAP - base_count
    half_count = EXPERTS // 2
    key_pairs, key_moves, key_order, key_rows = jax.random.split(jax.random.fold_in(key, 3), 4)
    pairing = jax.random.permutation(key_pairs, EXPERTS)
    moves = jax.random.randint(key_moves, (blocks, half_count), 0, spare + 1)
    moves = moves.at[:, 0].set(spare)
    paired = jnp.stack([base_count + moves, base_count - moves], axis=2).reshape(blocks, EXPERTS)
    counts = jnp.zeros((blocks, EXPERTS), jnp.int32).at[:, pairing].set(paired.astype(jnp.int32))
    orders = jax.vmap(expert_order)(jax.random.split(key_order, blocks))
    ordered_counts = jnp.take_along_axis(counts, orders, axis=1)
    bounds = jnp.cumsum(ordered_counts, axis=1)
    slot_pos = jnp.arange(slots_dev, dtype=jnp.int32)
    run_index = jnp.sum((bounds[:, None, :] <= slot_pos[None, :, None]).astype(jnp.int32), axis=2)
    expert_at = jnp.take_along_axis(orders, run_index, axis=1)
    route_grid = expert_at.reshape(blocks, TOPK, TOK_DEV).transpose(0, 2, 1)
    shuffles = jax.vmap(token_order)(jax.random.split(key_rows, blocks))
    route_grid = jnp.take_along_axis(route_grid, shuffles[:, :, None], axis=1)
    return route_grid.reshape(TOKENS, TOPK).astype(jnp.int32)


def close_gaps(values, router, routes, target_key):
    logits = jnp.dot(values, router, precision=lax.Precision.HIGHEST)
    expert_ids = jnp.arange(EXPERTS, dtype=jnp.int32)[None, :]
    first_hot = (routes[:, 0:1] == expert_ids).astype(jnp.float32)
    second_hot = (routes[:, 1:2] == expert_ids).astype(jnp.float32)
    diff_hot = first_hot - second_hot
    current_gap = jnp.sum(logits * diff_hot, axis=1)
    gram = jnp.dot(router.T, router, precision=lax.Precision.HIGHEST)
    diff_norm = jnp.sum(jnp.dot(diff_hot, gram, precision=lax.Precision.HIGHEST) * diff_hot, axis=1)
    target_gap = jax.random.uniform(target_key, (TOKENS,), jnp.float32, -2.5, 2.5)
    coefficient = (target_gap - current_gap) / diff_norm
    shift_rows = jnp.dot(coefficient[:, None] * diff_hot, router.T, precision=lax.Precision.HIGHEST)
    return values + shift_rows


def draw_router_weight(key, part):
    return router_table(key).astype(jnp.bfloat16)


def draw_route_ids(key, part):
    return route_table(key)


def draw_tokens(key, part):
    blocks = TOKENS // TOK_DEV
    groups = EXPERTS // EXP_DEV
    lanes = blocks // groups
    device = jnp.arange(TOKENS) // TOK_DEV
    along = (device % groups).astype(jnp.float32) / max(groups - 1, 1)
    across = (device // groups).astype(jnp.float32) / max(lanes - 1, 1)
    ramp_scale = (0.5 + 2.3 * along) * (1.0 + across)
    key_noise, key_scale = jax.random.split(jax.random.fold_in(key, 5), 2)
    key_target = jax.random.fold_in(key, 11)
    router = router_table(key)
    routes = route_table(key)
    spread = jnp.exp(jax.random.uniform(key_scale, (TOKENS,), jnp.float32, math.log(0.6), math.log(1.6)))
    noise_part = jax.random.normal(key_noise, (TOKENS, D), jnp.float32)
    values = noise_part * (ramp_scale * spread)[:, None]
    values = close_gaps(values, router, routes, key_target)
    return jnp.clip(values, -160.0, 160.0).astype(jnp.bfloat16)


def block_scale(key, shape, shards, smallest, top_value):
    loudness = 1.0
    for axis_at, shards_of in shards:
        heights = jax.random.uniform(jax.random.fold_in(jax.random.fold_in(key, 6), axis_at), (shards_of,), jnp.float32, smallest / len(shards), top_value / len(shards))
        loudness = loudness * jnp.repeat(jnp.exp(heights), shape[axis_at] // shards_of).reshape((-1,) + (1,) * (len(shape) - 1 - axis_at))
    return loudness


def scatter_about(stream_key, dims, scale, reach, cuts=(), kind=jnp.bfloat16):
    entries = jax.random.normal(stream_key, dims, jnp.float32) * scale
    if len(cuts) > 0:
        entries = block_scale(stream_key, dims, cuts, -0.22, 0.18) * entries
    return jnp.clip(entries, min=-reach, max=reach).astype(kind)


def setup_inputs(seed: int = 0) -> dict:
    keys = jax.random.split(jax.random.key(seed), 7)
    tokens = draw_tokens(jax.random.fold_in(keys[6], 71), 0)
    router_weight = draw_router_weight(jax.random.fold_in(keys[6], 71), 0)
    route_ids = draw_route_ids(jax.random.fold_in(keys[6], 71), 0)
    gate_weight = scatter_about(keys[3], (EXPERTS, FF, D), D ** -0.5, 0.125, ((0, 64), (1, 8)))
    up_weight = scatter_about(keys[4], (EXPERTS, FF, D), D ** -0.5, 0.125, ((0, 64), (1, 8)))
    down_weight = scatter_about(keys[5], (EXPERTS, FF, D), FF ** -0.5, 0.21875, ((0, 64), (1, 8)))
    return {"tokens": tokens, "router_weight": router_weight, "route_ids": route_ids, "gate_weight": gate_weight, "up_weight": up_weight, "down_weight": down_weight}


def block_tables(ids_block, weights_block):
    flat_ids = ids_block.reshape(-1)
    onehot = (flat_ids[:, None] == jnp.arange(EXPERTS, dtype=jnp.int32)[None, :]).astype(jnp.int32)
    before = jnp.cumsum(onehot, axis=0) - onehot
    position = jnp.sum(before * onehot, axis=1)
    slots = flat_ids * CAP + position
    slot_match = slots[None, :] == jnp.arange(EXPERTS * CAP, dtype=jnp.int32)[:, None]
    token_of = jnp.arange(TOK_DEV * TOPK, dtype=jnp.int32) // TOPK
    source_row = jnp.sum(jnp.where(slot_match, token_of[None, :], 0), axis=1).astype(jnp.int32)
    filled = jnp.any(slot_match, axis=1)
    flat_weights = weights_block.reshape(-1)
    slot_weight = jnp.sum(jnp.where(slot_match, flat_weights[None, :], jnp.zeros((), flat_weights.dtype)), axis=1)
    return source_row, filled, slot_weight


def tables_of(block_pair):
    return block_tables(block_pair[0], block_pair[1])


def reference(tokens, router_weight, route_ids, gate_weight, up_weight, down_weight):
    logits = jnp.dot(tokens, router_weight, preferred_element_type=jnp.float32)
    log_total = jax.nn.logsumexp(logits, axis=1)
    z_loss = jnp.mean(log_total * log_total)
    chosen = jnp.take_along_axis(logits, route_ids, axis=1)
    route_weight = jax.nn.softmax(chosen, axis=1)
    blocks = TOKENS // TOK_DEV
    source_row, filled, slot_weight = lax.map(tables_of, (route_ids.reshape(blocks, TOK_DEV, TOPK), route_weight.reshape(blocks, TOK_DEV, TOPK)))
    offsets = (jnp.arange(blocks, dtype=jnp.int32) * TOK_DEV)[:, None]
    global_row = (source_row + offsets).astype(jnp.int32)

    def by_expert(table):
        return table.reshape(blocks, EXPERTS, CAP).transpose(1, 0, 2).reshape(EXPERTS, blocks * CAP)

    def expert_step(accumulated, inputs):
        gate_one, up_one, down_one, rows_one, filled_one, weight_one = inputs
        expert_rows = jnp.where(filled_one[:, None], tokens[rows_one], jnp.zeros((), tokens.dtype))
        rows_wide = expert_rows.astype(jnp.float32)
        gate_val = jnp.dot(rows_wide, gate_one.astype(jnp.float32).T, preferred_element_type=jnp.float32)
        up_val = jnp.dot(rows_wide, up_one.astype(jnp.float32).T, preferred_element_type=jnp.float32)
        hidden = (jax.nn.silu(gate_val) * up_val).astype(jnp.bfloat16)
        expert_out = jnp.dot(hidden.astype(jnp.float32), down_one.astype(jnp.float32), preferred_element_type=jnp.float32).astype(jnp.bfloat16)
        accumulated = accumulated.at[rows_one].add(weight_one[:, None] * expert_out.astype(jnp.float32))
        return accumulated, None

    initial = jnp.zeros((TOKENS, D), jnp.float32)
    accumulated, unused = lax.scan(expert_step, initial, (gate_weight, up_weight, down_weight, by_expert(global_row), by_expert(filled), by_expert(slot_weight)))
    return accumulated.astype(jnp.bfloat16), z_loss
```

```python
import functools

import jax
import jax.numpy as jnp
from jax import lax
from jax.experimental import pallas as pl
from jax.experimental.pallas import tpu as pltpu
from jax.sharding import PartitionSpec as P

MESH = pl.DeviceIdType.MESH
BOTH = ("dp", "expert")
RING = 8
CAPACITY = 5
SEGS = 16
LANES = 128
BLOCK = CAPACITY * SEGS
SLOTS = RING * RING * CAPACITY
NT = (((1,), (1,)), ((), ()))
TN = (((0,), (0,)), ((), ()))
NN = (((1,), (0,)), ((), ()))
OFFSETS = (1, 7, 2, 6, 3, 5, 4)


def dot(a, b, dims):
    return lax.dot_general(a, b, dims, preferred_element_type=jnp.float32)


def kernel(
    tok,
    router,
    ids,
    gate,
    up,
    down,
    out,
    z_out,
    wide,
    send1,
    mid1,
    got1,
    rows,
    hidden,
    send2,
    mid2,
    got2,
    weights,
    zs1,
    zs2,
    zs3,
    zg1,
    zg2,
    zg3,
    load_sem,
    p_send,
    p_recv,
    zp_send,
    zp_recv,
    x_send,
    x_recv,
    d_send,
    d_recv,
):
    d = lax.axis_index("dp")
    e = lax.axis_index("expert")
    x, c = d // 2, lax.rem(d, 2)
    z, y = e // RING, lax.rem(e, RING)
    p = y * (1 - c) + z * c
    q = z * (1 - c) + y * c

    def on_p(v):
        return {"dp": d, "expert": (z * RING + v) * (1 - c) + (v * RING + y) * c}

    def on_q(v):
        return {"dp": d, "expert": (v * RING + y) * (1 - c) + (z * RING + v) * c}

    def at_dp(v):
        return {"dp": v, "expert": e}

    def shard(x_at, c_at):
        return 2 * lax.rem(x_at, 4) + c_at

    own, left, right, far = (shard(x + k, c) for k in (0, 3, 1, 2))

    barrier = pltpu.get_barrier_semaphore()
    for k in range(1, RING):
        pl.semaphore_signal(barrier, 1, device_id=on_p(lax.rem(p + k, RING)), device_id_type=MESH)
        pl.semaphore_signal(barrier, 1, device_id=on_q(lax.rem(q + k, RING)), device_id_type=MESH)
        pl.semaphore_signal(barrier, 1, device_id=at_dp(lax.rem(d + k, 8)), device_id_type=MESH)

    def piece(m, dev, first, count):
        start = pl.multiple_of(96 * dev + first, 16)
        return weights.at[m, pl.ds(start, count), :]

    loads = []
    for m, ref in enumerate((gate, up, down)):
        loads.append(pltpu.make_async_copy(ref.at[0], piece(m, own, 0, 96), load_sem.at[m]))
        loads[-1].start()

    logits = dot(tok[...], router[...], NN)
    top = jnp.max(logits, axis=1, keepdims=True)
    log_total = top + jnp.log(jnp.sum(jnp.exp(logits - top), axis=1, keepdims=True))
    local_sum = jnp.sum(log_total * log_total, axis=0, keepdims=True)
    zs1[...] = jnp.broadcast_to(local_sum, zs1.shape)
    zg1[p] = jnp.broadcast_to(local_sum, zs1.shape)
    tokens_here, experts = logits.shape
    lane = lax.broadcasted_iota(jnp.int32, (tokens_here, experts), 1)
    id0, id1 = ids[:, 0:1], ids[:, 1:2]
    hot0, hot1 = id0 == lane, id1 == lane
    chosen0 = jnp.sum(jnp.where(hot0, logits, 0.0), axis=1, keepdims=True)
    chosen1 = jnp.sum(jnp.where(hot1, logits, 0.0), axis=1, keepdims=True)
    peak = jnp.maximum(chosen0, chosen1)
    exp0, exp1 = jnp.exp(chosen0 - peak), jnp.exp(chosen1 - peak)
    weight0, weight1 = exp0 / (exp0 + exp1), exp1 / (exp0 + exp1)

    row_at = lax.broadcasted_iota(jnp.int32, (tokens_here, tokens_here), 0)
    col_at = lax.broadcasted_iota(jnp.int32, (tokens_here, tokens_here), 1)
    earlier = jnp.where(col_at < row_at, 1.0, 0.0).astype(jnp.bfloat16)
    one0 = jnp.where(hot0, 1.0, 0.0)
    one1 = jnp.where(hot1, 1.0, 0.0)
    before0 = dot(earlier, one0.astype(jnp.bfloat16), NN)
    before1 = dot(earlier, one1.astype(jnp.bfloat16), NN) + jnp.sum(one0, axis=0, keepdims=True)
    place0 = jnp.sum(before0 * one0, axis=1, keepdims=True).astype(jnp.int32)
    place1 = jnp.sum(before1 * one1, axis=1, keepdims=True).astype(jnp.int32)

    def ordinal(v):
        return jnp.where(c == 0, (v & 7) * RING + (v >> 3), v)

    slot0 = ordinal(id0) * CAPACITY + place0
    slot1 = ordinal(id1) * CAPACITY + place1
    slot_lane = lax.broadcasted_iota(jnp.int32, (tokens_here, SLOTS), 1)
    in0, in1 = slot0 == slot_lane, slot1 == slot_lane
    picks = jnp.where(in0 | in1, 1.0, 0.0).astype(jnp.bfloat16)
    mix = jnp.where(in0, weight0, jnp.where(in1, weight1, 0.0))
    mix_high = mix.astype(jnp.bfloat16)
    mix_low = (mix - mix_high.astype(jnp.float32)).astype(jnp.bfloat16)

    for n in range(8):
        chunk = dot(picks, tok[:, n * 256 : (n + 1) * 256], TN)
        wide[pl.ds(2 * n, SLOTS, stride=SEGS), :] = chunk[:, :LANES]
        wide[pl.ds(2 * n + 1, SLOTS, stride=SEGS), :] = chunk[:, LANES:]

    def narrow(dst):
        @pl.loop(0, RING)
        def _(a):
            for b in range(RING):
                start = pl.multiple_of((a * RING + b) * BLOCK, BLOCK)
                dst[a, b] = wide[pl.ds(start, BLOCK), :].astype(jnp.bfloat16)

    def to_rows(src):
        @pl.loop(0, RING)
        def _(a):
            for b in range(RING):
                start = pl.multiple_of((a * RING + b) * BLOCK, BLOCK)
                wide[pl.ds(start, BLOCK), :] = src[a, b].astype(jnp.float32)

        for j in range(SEGS):
            part = wide[pl.ds(j, SLOTS, stride=SEGS), :]
            rows[:, j * LANES : (j + 1) * LANES] = part.astype(jnp.bfloat16)

    narrow(send1)
    pl.semaphore_wait(barrier, 3 * (RING - 1))

    def step(phase, src, dst, me, peer):
        copies = []
        for k in OFFSETS:
            v = lax.rem(me + k, RING)
            copies.append(
                pltpu.make_async_remote_copy(
                    src.at[v],
                    dst(me),
                    p_send.at[phase, k],
                    p_recv.at[phase, k],
                    device_id=peer(v),
                    device_id_type=MESH,
                )
            )
            copies[-1].start()
        return copies

    def z_step(phase, src, dst, me, peer):
        copies = []
        for k in range(1, RING):
            v = lax.rem(me + k, RING)
            copies.append(
                pltpu.make_async_remote_copy(
                    src,
                    dst.at[me],
                    zp_send.at[phase, k],
                    zp_recv.at[phase, k],
                    device_id=peer(v),
                    device_id_type=MESH,
                )
            )
            copies[-1].start()
        return copies

    def finish(copies):
        for copy in copies:
            copy.wait()

    def along(m, go_right, stage):
        if go_right:
            dev, first = (own, 0) if stage == 0 else (own, 48) if stage == 1 else (left, 0)
        else:
            dev, first = (own, 48) if stage == 0 else (own, 0) if stage == 1 else (right, 48)
        side = 0 if go_right else 1
        return pltpu.make_async_remote_copy(
            piece(m, dev, first, 48),
            piece(m, dev, first, 48),
            x_send.at[side, m, stage],
            x_recv.at[side, m, stage],
            device_id=at_dp(right if go_right else left),
            device_id_type=MESH,
        )

    def across(m, which):
        dev = (own, left, right, far)[which]
        return pltpu.make_async_remote_copy(
            piece(m, dev, 0, 96),
            piece(m, dev, 0, 96),
            d_send.at[m, which],
            d_recv.at[m, which],
            device_id=at_dp(x * 2 + 1 - c),
            device_id_type=MESH,
        )

    sent = []

    def go(copy):
        copy.start()
        sent.append(copy)

    def own_along(m):
        for stage in (0, 1):
            go(along(m, True, stage))
            go(along(m, False, stage))

    def relay(m):
        along(m, True, 0).wait_recv()
        go(along(m, True, 2))
        along(m, False, 0).wait_recv()
        go(along(m, False, 2))

    def pass_neighbours(m):
        along(m, True, 1).wait_recv()
        go(across(m, 1))
        along(m, False, 1).wait_recv()
        go(across(m, 2))

    def pass_far(m):
        along(m, True, 2).wait_recv()
        along(m, False, 2).wait_recv()
        go(across(m, 3))

    def arrived(m):
        for which in range(4):
            across(m, which).wait_recv()

    for load in loads:
        load.wait()
    own_along(0)
    own_along(1)
    first = step(0, send1, lambda me: mid1.at[:, me], p, on_p)
    z_first = z_step(0, zs1, zg1, p, on_p)
    for m in range(3):
        go(across(m, 0))
    mid1[:, p] = send1[p]
    finish(first)
    finish(z_first)
    z_row = jnp.sum(zg1[...], axis=0)
    zs2[...] = z_row
    zg2[q] = z_row
    second = step(1, mid1, lambda me: got1.at[me], q, on_q)
    relay(0)
    relay(1)
    own_along(2)
    pass_neighbours(0)
    pass_neighbours(1)
    z_second = z_step(1, zs2, zg2, q, on_q)
    got1[q] = mid1[q]
    finish(second)
    finish(z_second)
    z_plane = jnp.sum(zg2[...], axis=0)
    zs3[...] = z_plane
    zg3[d] = z_plane
    relay(2)
    pass_neighbours(2)
    to_rows(got1)
    z_third = z_step(2, zs3, zg3, d, at_dp)
    pass_far(0)
    pass_far(1)
    arrived(0)
    arrived(1)
    for n in range(3):
        cut = slice(n * 256, (n + 1) * 256)
        gated = dot(rows[...], weights[0, cut, :], NT)
        upped = dot(rows[...], weights[1, cut, :], NT)
        hidden[:, cut] = (gated / (1.0 + jnp.exp(-gated)) * upped).astype(jnp.bfloat16)
    pass_far(2)
    arrived(2)
    for n in range(8):
        chunk = dot(hidden[...], weights[2, :, n * 256 : (n + 1) * 256], NN)
        wide[pl.ds(2 * n, SLOTS, stride=SEGS), :] = chunk[:, :LANES]
        wide[pl.ds(2 * n + 1, SLOTS, stride=SEGS), :] = chunk[:, LANES:]
    narrow(send2)
    finish(z_third)
    total = jnp.sum(zg3[...], axis=0)
    z_out[...] = total[0:1, 0:1] / jnp.float32(tokens_here * 512)
    third = step(2, send2, lambda me: mid2.at[:, me], q, on_q)
    mid2[:, q] = send2[q]
    finish(third)
    fourth = step(3, mid2, lambda me: got2.at[me], p, on_p)
    got2[p] = mid2[p]
    for copy in sent:
        copy.wait_send()
    finish(fourth)
    to_rows(got2)
    for n in range(8):
        cut = slice(n * 256, (n + 1) * 256)
        part = rows[:, cut]
        out[:, cut] = (dot(mix_high, part, NN) + dot(mix_low, part, NN)).astype(jnp.bfloat16)


def on_device(tokens, router_weight, route_ids, gate_weight, up_weight, down_weight):
    rows_here, width = tokens.shape
    blocks = (RING, RING, BLOCK, LANES)
    bf16, f32 = jnp.bfloat16, jnp.float32
    vmem = pl.BlockSpec(memory_space=pltpu.VMEM)
    hbm = pl.BlockSpec(memory_space=pl.ANY)
    small = (8, LANES)
    dma = pltpu.SemaphoreType.DMA
    mixture, z_loss = pl.pallas_call(
        kernel,
        out_shape=(
            jax.ShapeDtypeStruct((rows_here, width), bf16),
            jax.ShapeDtypeStruct((1, 1), f32),
        ),
        in_specs=[vmem, vmem, vmem, hbm, hbm, hbm],
        out_specs=(vmem, vmem),
        scratch_shapes=[
            pltpu.VMEM((SLOTS * SEGS, LANES), f32),
            pltpu.VMEM(blocks, bf16),
            pltpu.VMEM(blocks, bf16),
            pltpu.VMEM(blocks, bf16),
            pltpu.VMEM((SLOTS, width), bf16),
            pltpu.VMEM((SLOTS, 768), bf16),
            pltpu.VMEM(blocks, bf16),
            pltpu.VMEM(blocks, bf16),
            pltpu.VMEM(blocks, bf16),
            pltpu.VMEM((3, 768, width), bf16),
            pltpu.VMEM(small, f32),
            pltpu.VMEM(small, f32),
            pltpu.VMEM(small, f32),
            pltpu.VMEM((8,) + small, f32),
            pltpu.VMEM((8,) + small, f32),
            pltpu.VMEM((8,) + small, f32),
            dma((3,)),
            dma((4, RING)),
            dma((4, RING)),
            dma((3, RING)),
            dma((3, RING)),
            dma((2, 3, 3)),
            dma((2, 3, 3)),
            dma((3, 4)),
            dma((3, 4)),
        ],
        compiler_params=pltpu.CompilerParams(
            collective_id=0, has_side_effects=True, vmem_limit_bytes=60 * 1024 * 1024
        ),
    )(tokens, router_weight, route_ids, gate_weight, up_weight, down_weight)
    return mixture, z_loss.reshape(())


def solution(mesh):
    return jax.shard_map(
        on_device,
        mesh=mesh,
        in_specs=(
            P(BOTH, None),
            P(),
            P(BOTH, None),
            P("expert", "dp", None),
            P("expert", "dp", None),
            P("expert", "dp", None),
        ),
        out_specs=(P(BOTH, None), P()),
        check_vma=False,
    )
```

```python
import jax
import jax.numpy as jnp
from jax import lax
from jax.experimental import pallas as pl
from jax.experimental.pallas import tpu as pltpu
from jax.sharding import PartitionSpec as P

MESH = pl.DeviceIdType.MESH
BOTH = ("dp", "expert")
RING = 8
CAPACITY = 5
HALVES = 2
SEGS = 8
LANES = 128
HALF = SEGS * LANES
BLOCK = CAPACITY * SEGS
SLOTS = RING * RING * CAPACITY
FF = 768
NT = (((1,), (1,)), ((), ()))
NN = (((1,), (0,)), ((), ()))
OFFSETS = (4, 3, 5, 2, 6, 1, 7)
scope = jax.named_scope


def dot(a, b, dims):
    return lax.dot_general(a, b, dims, preferred_element_type=jnp.float32)


def kernel(
    tok_hbm,
    router_hbm,
    ids_hbm,
    gate,
    up,
    down,
    out,
    z_out,
    tok,
    router,
    ids,
    wide,
    send1,
    mid1,
    got1,
    rows,
    acc,
    hidden,
    send2,
    mid2,
    got2,
    gate_up,
    downs,
    mixture,
    mix_high,
    mix_low,
    zs1,
    zs2,
    zs3,
    zg1,
    zg2,
    zg3,
    load_sem,
    e_send,
    e_recv,
    z_send,
    z_recv,
    x_send,
    x_recv,
    d_send,
    d_recv,
):
    d = lax.axis_index("dp")
    e = lax.axis_index("expert")
    x, c = d // 2, lax.rem(d, 2)
    z, y = e // RING, lax.rem(e, RING)
    p = y * (1 - c) + z * c
    q = z * (1 - c) + y * c

    def on_p(v):
        return {"dp": d, "expert": (z * RING + v) * (1 - c) + (v * RING + y) * c}

    def on_q(v):
        return {"dp": d, "expert": (v * RING + y) * (1 - c) + (z * RING + v) * c}

    def at_dp(v):
        return {"dp": v, "expert": e}

    def shard(x_at, c_at):
        return 2 * lax.rem(x_at, 4) + c_at

    own, left, right, far = (shard(x + k, c) for k in (0, 3, 1, 2))

    barrier = pltpu.get_barrier_semaphore()
    for k in range(1, RING):
        pl.semaphore_signal(barrier, 1, device_id=on_p(lax.rem(p + k, RING)), device_id_type=MESH)
        pl.semaphore_signal(barrier, 1, device_id=on_q(lax.rem(q + k, RING)), device_id_type=MESH)
        pl.semaphore_signal(barrier, 1, device_id=at_dp(lax.rem(d + k, 8)), device_id_type=MESH)

    inputs = []
    for m, (src, dst) in enumerate(((tok_hbm, tok), (router_hbm, router), (ids_hbm, ids))):
        inputs.append(pltpu.make_async_copy(src, dst, load_sem.at[4 + m]))
        inputs[-1].start()

    def piece(m, dev, first, count):
        part = pl.ds(pl.multiple_of(96 * dev + first, 16), count)
        return gate_up.at[m, part, :] if m < 2 else downs.at[m - 2, part, :]

    loads = []
    for m in range(4):
        src = (gate.at[0], up.at[0], down.at[0, :, 0:HALF], down.at[0, :, HALF:])[m]
        loads.append(pltpu.make_async_copy(src, piece(m, own, 0, 96), load_sem.at[m]))
        loads[-1].start()

    inputs[2].wait()
    experts, tokens_here = router.shape[0], tok.shape[0]
    expert_at = lax.broadcasted_iota(jnp.int32, (experts, tokens_here), 0)
    id0, id1 = ids[0:1, :], ids[1:2, :]
    hot0, hot1 = id0 == expert_at, id1 == expert_at

    row_at = lax.broadcasted_iota(jnp.int32, (tokens_here, tokens_here), 0)
    col_at = lax.broadcasted_iota(jnp.int32, (tokens_here, tokens_here), 1)
    earlier = jnp.where(row_at < col_at, 1.0, 0.0).astype(jnp.bfloat16)
    one0 = jnp.where(hot0, 1.0, 0.0)
    one1 = jnp.where(hot1, 1.0, 0.0)
    before0 = dot(one0.astype(jnp.bfloat16), earlier, NN)
    before1 = dot(one1.astype(jnp.bfloat16), earlier, NN) + jnp.sum(one0, axis=1, keepdims=True)
    place0 = jnp.sum(before0 * one0, axis=0, keepdims=True).astype(jnp.int32)
    place1 = jnp.sum(before1 * one1, axis=0, keepdims=True).astype(jnp.int32)

    def ordinal(v):
        return jnp.where(c == 0, (v & 7) * RING + (v >> 3), v)

    slot0 = ordinal(id0) * CAPACITY + place0
    slot1 = ordinal(id1) * CAPACITY + place1
    slot_at = lax.broadcasted_iota(jnp.int32, (SLOTS, tokens_here), 0)
    in0, in1 = slot0 == slot_at, slot1 == slot_at
    picks = jnp.where(in0 | in1, 1.0, 0.0).astype(jnp.bfloat16)

    def narrow(dst):
        @pl.loop(0, RING)
        def _(a):
            for b in range(RING):
                start = pl.multiple_of((a * RING + b) * BLOCK, BLOCK)
                dst[a, b] = wide[pl.ds(start, BLOCK), :].astype(jnp.bfloat16)

    def spread(n, chunk):
        for i in range(2):
            wide[pl.ds(2 * n + i, SLOTS, stride=SEGS), :] = chunk[:, i * LANES : (i + 1) * LANES]

    def to_rows(src, h):
        @pl.loop(0, RING)
        def _(a):
            for b in range(RING):
                start = pl.multiple_of((a * RING + b) * BLOCK, BLOCK)
                wide[pl.ds(start, BLOCK), :] = src[h, a, b].astype(jnp.float32)

        for j in range(SEGS):
            part = wide[pl.ds(j, SLOTS, stride=SEGS), :]
            cut = slice(h * HALF + j * LANES, h * HALF + (j + 1) * LANES)
            rows[:, cut] = part.astype(jnp.bfloat16)

    def exchange(phase, h, src, dst, me, peer):
        for k in OFFSETS:
            v = lax.rem(me + k, RING)
            pltpu.make_async_remote_copy(
                src.at[h, v],
                dst,
                e_send.at[phase, h],
                e_recv.at[phase, h],
                device_id=peer(v),
                device_id_type=MESH,
            ).start()

    def wait_for(ref, sem):
        pltpu.make_async_copy(ref, ref, sem).wait()

    def landed(phase, h):
        wait_for(send1.at[h, pl.ds(0, RING - 1)], e_recv.at[phase, h])

    def out_of(phase, h):
        wait_for(send1.at[h, pl.ds(0, RING - 1)], e_send.at[phase, h])

    def z_exchange(phase, src, dst, me, peer):
        for k in range(1, RING):
            v = lax.rem(me + k, RING)
            pltpu.make_async_remote_copy(
                src,
                dst.at[me],
                z_send.at[phase],
                z_recv.at[phase],
                device_id=peer(v),
                device_id_type=MESH,
            ).start()

    def z_landed(phase):
        wait_for(zg1.at[pl.ds(0, RING - 1)], z_recv.at[phase])

    def along(m, go_right, stage):
        if go_right:
            dev, first = (own, 0) if stage == 0 else (own, 48) if stage == 1 else (left, 0)
        else:
            dev, first = (own, 48) if stage == 0 else (own, 0) if stage == 1 else (right, 48)
        side = 0 if go_right else 1
        return pltpu.make_async_remote_copy(
            piece(m, dev, first, 48),
            piece(m, dev, first, 48),
            x_send.at[m],
            x_recv.at[side, m, stage],
            device_id=at_dp(right if go_right else left),
            device_id_type=MESH,
        )

    def across(m, which):
        dev = (own, left, right, far)[which]
        return pltpu.make_async_remote_copy(
            piece(m, dev, 0, 96),
            piece(m, dev, 0, 96),
            d_send.at[m],
            d_recv.at[m],
            device_id=at_dp(x * 2 + 1 - c),
            device_id_type=MESH,
        )

    def go(copy):
        copy.start()

    def own_along(m, stage):
        go(along(m, True, stage))
        go(along(m, False, stage))

    def relay(m):
        along(m, True, 0).wait_recv()
        go(along(m, True, 2))
        along(m, False, 0).wait_recv()
        go(along(m, False, 2))

    def pass_neighbours(m):
        along(m, True, 1).wait_recv()
        go(across(m, 1))
        along(m, False, 1).wait_recv()
        go(across(m, 2))

    def pass_far(m):
        along(m, True, 2).wait_recv()
        along(m, False, 2).wait_recv()
        go(across(m, 3))

    def rows_of(m, count):
        return gate_up.at[m, pl.ds(0, count)] if m < 2 else downs.at[m - 2, pl.ds(0, count)]

    def arrived(m):
        wait_for(rows_of(m, 4 * 96), d_recv.at[m])

    def dispatch(h):
        for n in range(SEGS // 2):
            cut = slice(h * HALF + n * 256, h * HALF + (n + 1) * 256)
            spread(n, dot(picks, tok[:, cut], NN))
        narrow(send1.at[h])

    inputs[0].wait()
    with scope("dispatch0"):
        dispatch(0)
    with scope("barrier"):
        pl.semaphore_wait(barrier, 3 * (RING - 1))
    for load in loads:
        load.wait()
    for m in range(2):
        own_along(m, 0)
        own_along(m, 1)
    exchange(0, 0, send1, mid1.at[0, :, p], p, on_p)
    with scope("dispatch1"):
        dispatch(1)
    inputs[1].wait()
    exchange(0, 1, send1, mid1.at[1, :, p], p, on_p)
    for m in range(4):
        go(across(m, 0))
    with scope("router"):
        for h in range(HALVES):
            mid1[h, :, p] = send1[h, p]
        logits = dot(router[...], tok[...], NT)
        top = jnp.max(logits, axis=0, keepdims=True)
        log_total = top + jnp.log(jnp.sum(jnp.exp(logits - top), axis=0, keepdims=True))
        local_sum = jnp.sum(log_total * log_total, axis=1, keepdims=True)
        zs1[...] = jnp.broadcast_to(local_sum, zs1.shape)
        zg1[p] = jnp.broadcast_to(local_sum, zs1.shape)
        chosen0 = jnp.sum(jnp.where(hot0, logits, 0.0), axis=0, keepdims=True)
        chosen1 = jnp.sum(jnp.where(hot1, logits, 0.0), axis=0, keepdims=True)
        peak = jnp.maximum(chosen0, chosen1)
        exp0, exp1 = jnp.exp(chosen0 - peak), jnp.exp(chosen1 - peak)
        weight0, weight1 = exp0 / (exp0 + exp1), exp1 / (exp0 + exp1)
        mix = jnp.where(in0, weight0, jnp.where(in1, weight1, 0.0)).T
        mix_high[...] = mix.astype(jnp.bfloat16)
        mix_low[...] = (mix - mix.astype(jnp.bfloat16).astype(jnp.float32)).astype(jnp.bfloat16)
    with scope("relay_g"):
        relay(0)
    z_exchange(0, zs1, zg1, p, on_p)
    with scope("p1_0"):
        landed(0, 0)
    with scope("p1_1s"):
        out_of(0, 1)
    exchange(1, 0, mid1, got1.at[0, q], q, on_q)
    with scope("relay_u"):
        relay(1)
        pass_neighbours(0)
    with scope("p1_1"):
        landed(0, 1)
    exchange(1, 1, mid1, got1.at[1, q], q, on_q)
    own_along(2, 0)
    own_along(2, 1)
    for h in range(HALVES):
        got1[h, q] = mid1[h, q]
    with scope("pass_u"):
        pass_neighbours(1)
    with scope("far_g"):
        pass_far(0)
    z_landed(0)
    z_row = jnp.sum(zg1[...], axis=0)
    zs2[...] = z_row
    zg2[q] = z_row
    with scope("p2_0"):
        landed(1, 0)
    with scope("rows_0"):
        to_rows(got1, 0)
    z_exchange(1, zs2, zg2, q, on_q)
    with scope("far_u"):
        pass_far(1)
    with scope("relay_d0"):
        relay(2)
    own_along(3, 0)
    own_along(3, 1)

    def project(h, m, n):
        across_k = slice(h * HALF, (h + 1) * HALF)
        return dot(rows[:, across_k], gate_up[m, n * 256 : (n + 1) * 256, across_k], NT)

    for m in range(2):
        with scope("arrived_%d" % m):
            arrived(m)
        with scope("ffn_0%d" % m):
            for n in range(FF // 256):
                acc[m, :, n * 256 : (n + 1) * 256] = project(0, m, n)
    with scope("pass_d0"):
        pass_neighbours(2)
    with scope("p2_1"):
        landed(1, 1)
    with scope("rows_1"):
        to_rows(got1, 1)
    with scope("far_d0"):
        pass_far(2)
    with scope("ffn_1"):
        for n in range(FF // 256):
            cut = slice(n * 256, (n + 1) * 256)
            gated = acc[0, :, cut] + project(1, 0, n)
            upped = acc[1, :, cut] + project(1, 1, n)
            hidden[:, cut] = (gated / (1.0 + jnp.exp(-gated)) * upped).astype(jnp.bfloat16)
    for h in range(HALVES):
        with scope("far_d%d" % h):
            if h == 1:
                relay(3)
                pass_neighbours(3)
                pass_far(3)
        with scope("arrived_d%d" % h):
            arrived(2 + h)
        with scope("down_%d" % h):
            for n in range(SEGS // 2):
                spread(n, dot(hidden[...], downs[h, :, n * 256 : (n + 1) * 256], NN))
            narrow(send2.at[h])
        exchange(2, h, send2, mid2.at[h, :, q], q, on_q)
    z_landed(1)
    z_plane = jnp.sum(zg2[...], axis=0)
    zs3[...] = z_plane
    zg3[d] = z_plane
    for h in range(HALVES):
        mid2[h, :, q] = send2[h, q]
    z_exchange(2, zs3, zg3, d, at_dp)
    with scope("p3_0"):
        landed(2, 0)
    with scope("p3_1s"):
        out_of(2, 1)
    exchange(3, 0, mid2, got2.at[0, p], p, on_p)
    z_landed(2)
    total = jnp.sum(zg3[...], axis=0)
    z_out[...] = total[0:1, 0:1] / jnp.float32(tokens_here * 512)
    with scope("p3_1"):
        landed(2, 1)
    exchange(3, 1, mid2, got2.at[1, p], p, on_p)
    for h in range(HALVES):
        got2[h, p] = mid2[h, p]
    with scope("outs"):
        out_of(0, 0)
        out_of(1, 0)
        out_of(1, 1)
        out_of(2, 0)
        for phase in range(3):
            wait_for(zg1.at[pl.ds(0, RING - 1)], z_send.at[phase])
        for m in range(4):
            wait_for(rows_of(m, 6 * 48), x_send.at[m])
            wait_for(rows_of(m, 4 * 96), d_send.at[m])
    stores = []
    for h in range(HALVES):
        with scope("p4_%d" % h):
            landed(3, h)
        with scope("rows2_%d" % h):
            to_rows(got2, h)
        with scope("mix_%d" % h):
            for n in range(SEGS // 2):
                cut = slice(h * HALF + n * 256, h * HALF + (n + 1) * 256)
                part = rows[:, cut]
                mixed = dot(mix_high[...], part, NN) + dot(mix_low[...], part, NN)
                mixture[:, cut] = mixed.astype(jnp.bfloat16)
        cut = slice(h * HALF, (h + 1) * HALF)
        stores.append(pltpu.make_async_copy(mixture.at[:, cut], out.at[:, cut], load_sem.at[h]))
        stores[-1].start()
    with scope("end"):
        out_of(3, 0)
        out_of(3, 1)
        for store in stores:
            store.wait()


def on_device(tokens, router_weight, route_ids, gate_weight, up_weight, down_weight):
    rows_here, width = tokens.shape
    blocks = (HALVES, RING, RING, BLOCK, LANES)
    bf16, f32 = jnp.bfloat16, jnp.float32
    vmem = pl.BlockSpec(memory_space=pltpu.VMEM)
    hbm = pl.BlockSpec(memory_space=pltpu.HBM)
    small = (8, LANES)
    dma = pltpu.SemaphoreType.DMA
    mixture, z_loss = pl.pallas_call(
        kernel,
        out_shape=(
            jax.ShapeDtypeStruct((rows_here, width), bf16),
            jax.ShapeDtypeStruct((1, 1), f32),
        ),
        in_specs=[hbm] * 6,
        out_specs=(hbm, vmem),
        scratch_shapes=[
            pltpu.VMEM((rows_here, width), bf16),
            pltpu.VMEM(router_weight.shape[::-1], bf16),
            pltpu.VMEM(route_ids.shape[::-1], jnp.int32),
            pltpu.VMEM((SLOTS * SEGS, LANES), f32),
            pltpu.VMEM(blocks, bf16),
            pltpu.VMEM(blocks, bf16),
            pltpu.VMEM(blocks, bf16),
            pltpu.VMEM((SLOTS, width), bf16),
            pltpu.VMEM((2, SLOTS, FF), f32),
            pltpu.VMEM((SLOTS, FF), bf16),
            pltpu.VMEM(blocks, bf16),
            pltpu.VMEM(blocks, bf16),
            pltpu.VMEM(blocks, bf16),
            pltpu.VMEM((2, FF, width), bf16),
            pltpu.VMEM((HALVES, FF, HALF), bf16),
            pltpu.VMEM((rows_here, width), bf16),
            pltpu.VMEM((rows_here, SLOTS), bf16),
            pltpu.VMEM((rows_here, SLOTS), bf16),
            pltpu.VMEM(small, f32),
            pltpu.VMEM(small, f32),
            pltpu.VMEM(small, f32),
            pltpu.VMEM((8,) + small, f32),
            pltpu.VMEM((8,) + small, f32),
            pltpu.VMEM((8,) + small, f32),
            dma((7,)),
            dma((4, HALVES)),
            dma((4, HALVES)),
            dma((3,)),
            dma((3,)),
            dma((4,)),
            dma((2, 4, 3)),
            dma((4,)),
            dma((4,)),
        ],
        compiler_params=pltpu.CompilerParams(
            collective_id=0, has_side_effects=True, vmem_limit_bytes=60 * 1024 * 1024
        ),
    )(tokens, router_weight.T, route_ids.T, gate_weight, up_weight, down_weight)
    return mixture, z_loss.reshape(())


def solution(mesh):
    return jax.shard_map(
        on_device,
        mesh=mesh,
        in_specs=(
            P(BOTH, None),
            P(),
            P(BOTH, None),
            P("expert", "dp", None),
            P("expert", "dp", None),
            P("expert", "dp", None),
        ),
        out_specs=(P(BOTH, None), P()),
        check_vma=False,
    )
```

```python
import jax
import jax.numpy as jnp
from jax import lax
from jax.experimental import pallas as pl
from jax.experimental.pallas import tpu as pltpu
from jax.sharding import PartitionSpec as P

MESH = pl.DeviceIdType.MESH
BOTH = ("dp", "expert")
RING = 8
CAPACITY = 5
HALVES = 2
SEGS = 8
LANES = 128
HALF = SEGS * LANES
BLOCK = CAPACITY * SEGS
SLOTS = RING * RING * CAPACITY
FF = 768
NT = (((1,), (1,)), ((), ()))
NN = (((1,), (0,)), ((), ()))
OFFSETS = (4, 3, 5, 2, 6, 1, 7)
EARLY = OFFSETS[:5]
scope = jax.named_scope


def dot(a, b, dims):
    return lax.dot_general(a, b, dims, preferred_element_type=jnp.float32)


def kernel(
    tok_hbm,
    router_hbm,
    ids_hbm,
    gate,
    up,
    down,
    out,
    z_out,
    tok,
    router,
    ids,
    wide,
    send1,
    mid1,
    got1,
    rows,
    acc,
    hidden,
    send2,
    mid2,
    got2,
    gate_up,
    downs,
    mixture,
    mix_high,
    mix_low,
    z_val,
    zs1,
    zs2,
    zs3,
    zg1,
    zg2,
    zg3,
    load_sem,
    e_send,
    e_recv,
    z_send,
    z_recv,
    x_send,
    x_recv,
    d_send,
    d_recv,
    line,
    plane,
):
    d = lax.axis_index("dp")
    e = lax.axis_index("expert")
    x, c = d // 2, lax.rem(d, 2)
    z, y = e // RING, lax.rem(e, RING)
    p = y * (1 - c) + z * c
    q = z * (1 - c) + y * c

    def on_p(v):
        return {"dp": d, "expert": (z * RING + v) * (1 - c) + (v * RING + y) * c}

    def on_q(v):
        return {"dp": d, "expert": (v * RING + y) * (1 - c) + (z * RING + v) * c}

    def at_dp(v):
        return {"dp": v, "expert": e}

    def shard(x_at, c_at):
        return 2 * lax.rem(x_at, 4) + c_at

    own, left, right, far = (shard(x + k, c) for k in (0, 3, 1, 2))

    inputs = []
    for m, (src, dst) in enumerate(((ids_hbm, ids), (tok_hbm, tok), (router_hbm, router))):
        inputs.append(pltpu.make_async_copy(src, dst, load_sem.at[4 + m]))
        inputs[-1].start()

    barrier = pltpu.get_barrier_semaphore()
    other = at_dp(x * 2 + 1 - c)
    for k in OFFSETS:
        for peer in (z * RING + lax.rem(y + k, RING), lax.rem(z + k, RING) * RING + y):
            pl.semaphore_signal(
                barrier, 1, device_id={"dp": x * 2 + 1, "expert": peer}, device_id_type=MESH
            )
    for k in range(1, 4):
        pl.semaphore_signal(barrier, 1, device_id=at_dp(shard(x + k, 0)), device_id_type=MESH)

    @pl.when(c == 1)
    def _():
        pl.semaphore_signal(barrier, 1, device_id=other, device_id_type=MESH)

    def line_here():
        @pl.when(c == 0)
        def _():
            pl.semaphore_wait(barrier, 7)
            pl.semaphore_signal(line, 1, device_id=other, device_id_type=MESH)

        @pl.when(c == 1)
        def _():
            pl.semaphore_wait(line, 1)

    def plane_here():
        @pl.when(c == 1)
        def _():
            pl.semaphore_wait(barrier, 4 * (RING - 1))
            pl.semaphore_signal(plane, 1, device_id=other, device_id_type=MESH)

        @pl.when(c == 0)
        def _():
            pl.semaphore_wait(plane, 1)

    def piece(m, dev, first, count):
        part = pl.ds(pl.multiple_of(96 * dev + first, 16), count)
        return gate_up.at[m, part, :] if m < 2 else downs.at[m - 2, part, :]

    loads = []
    for m in range(4):
        src = (gate.at[0], up.at[0], down.at[0, :, 0:HALF], down.at[0, :, HALF:])[m]
        loads.append(pltpu.make_async_copy(src, piece(m, own, 0, 96), load_sem.at[m]))
        loads[-1].start()

    with scope("ids_wait"):
        inputs[0].wait()
    experts, tokens_here = router.shape[0], tok.shape[0]
    expert_at = lax.broadcasted_iota(jnp.int32, (experts, tokens_here), 0)
    id0, id1 = ids[0:1, :], ids[1:2, :]
    hot0, hot1 = id0 == expert_at, id1 == expert_at

    row_at = lax.broadcasted_iota(jnp.int32, (tokens_here, tokens_here), 0)
    col_at = lax.broadcasted_iota(jnp.int32, (tokens_here, tokens_here), 1)
    earlier = jnp.where(row_at < col_at, 1.0, 0.0).astype(jnp.bfloat16)
    one0 = jnp.where(hot0, 1.0, 0.0)
    one1 = jnp.where(hot1, 1.0, 0.0)
    before0 = dot(one0.astype(jnp.bfloat16), earlier, NN)
    before1 = dot(one1.astype(jnp.bfloat16), earlier, NN) + jnp.sum(one0, axis=1, keepdims=True)
    place0 = jnp.sum(before0 * one0, axis=0, keepdims=True).astype(jnp.int32)
    place1 = jnp.sum(before1 * one1, axis=0, keepdims=True).astype(jnp.int32)

    def ordinal(v):
        return jnp.where(c == 0, (v & 7) * RING + (v >> 3), v)

    slot0 = ordinal(id0) * CAPACITY + place0
    slot1 = ordinal(id1) * CAPACITY + place1
    slot_at = lax.broadcasted_iota(jnp.int32, (SLOTS, tokens_here), 0)
    in0, in1 = slot0 == slot_at, slot1 == slot_at
    picks = jnp.where(in0 | in1, 1.0, 0.0).astype(jnp.bfloat16)

    def narrow(dst):
        @pl.loop(0, RING)
        def _(a):
            for b in range(RING):
                start = pl.multiple_of((a * RING + b) * BLOCK, BLOCK)
                dst[a, b] = wide[pl.ds(start, BLOCK), :].astype(jnp.bfloat16)

    def spread(n, chunk):
        for i in range(2):
            wide[pl.ds(2 * n + i, SLOTS, stride=SEGS), :] = chunk[:, i * LANES : (i + 1) * LANES]

    def to_rows(src, h):
        @pl.loop(0, RING)
        def _(a):
            for b in range(RING):
                start = pl.multiple_of((a * RING + b) * BLOCK, BLOCK)
                wide[pl.ds(start, BLOCK), :] = src[h, a, b].astype(jnp.float32)

        for j in range(SEGS):
            part = wide[pl.ds(j, SLOTS, stride=SEGS), :]
            cut = slice(h * HALF + j * LANES, h * HALF + (j + 1) * LANES)
            rows[:, cut] = part.astype(jnp.bfloat16)

    def exchange(phase, h, src, dst, me, peer):
        for k in OFFSETS:
            v = lax.rem(me + k, RING)
            pltpu.make_async_remote_copy(
                src.at[h, v],
                dst,
                e_send.at[phase, h, 0 if k in EARLY else 1],
                e_recv.at[phase, h],
                device_id=peer(v),
                device_id_type=MESH,
            ).start()

    def wait_for(ref, sem):
        pltpu.make_async_copy(ref, ref, sem).wait()

    def landed(phase, h):
        wait_for(send1.at[h, pl.ds(0, RING - 1)], e_recv.at[phase, h])

    def early_out(phase, h):
        wait_for(send1.at[h, pl.ds(0, len(EARLY))], e_send.at[phase, h, 0])

    def late_out(phase, h):
        if len(EARLY) == RING - 1:
            return
        wait_for(send1.at[h, pl.ds(0, RING - 1 - len(EARLY))], e_send.at[phase, h, 1])

    def out_of(phase, h):
        early_out(phase, h)
        late_out(phase, h)

    def z_exchange(phase, src, dst, me, peer):
        for k in range(1, RING):
            v = lax.rem(me + k, RING)
            pltpu.make_async_remote_copy(
                src,
                dst.at[me],
                z_send.at[phase],
                z_recv.at[phase],
                device_id=peer(v),
                device_id_type=MESH,
            ).start()

    def z_landed(phase):
        wait_for(zg1.at[pl.ds(0, RING - 1)], z_recv.at[phase])

    def along(m, go_right, stage):
        if go_right:
            dev, first = (own, 0) if stage == 0 else (own, 48) if stage == 1 else (left, 0)
        else:
            dev, first = (own, 48) if stage == 0 else (own, 0) if stage == 1 else (right, 48)
        side = 0 if go_right else 1
        return pltpu.make_async_remote_copy(
            piece(m, dev, first, 48),
            piece(m, dev, first, 48),
            x_send.at[m],
            x_recv.at[side, m, stage],
            device_id=at_dp(right if go_right else left),
            device_id_type=MESH,
        )

    def across(m, which):
        dev = (own, left, right, far)[which]
        return pltpu.make_async_remote_copy(
            piece(m, dev, 0, 96),
            piece(m, dev, 0, 96),
            d_send.at[m],
            d_recv.at[m],
            device_id=at_dp(x * 2 + 1 - c),
            device_id_type=MESH,
        )

    def go(copy):
        copy.start()

    def own_along(m, stage):
        go(along(m, True, stage))
        go(along(m, False, stage))

    def relay(m):
        along(m, True, 0).wait_recv()
        go(along(m, True, 2))
        along(m, False, 0).wait_recv()
        go(along(m, False, 2))

    def pass_neighbours(m):
        along(m, True, 1).wait_recv()
        go(across(m, 1))
        along(m, False, 1).wait_recv()
        go(across(m, 2))

    def pass_far(m):
        along(m, True, 2).wait_recv()
        along(m, False, 2).wait_recv()
        go(across(m, 3))

    def rows_of(m, count):
        return gate_up.at[m, pl.ds(0, count)] if m < 2 else downs.at[m - 2, pl.ds(0, count)]

    def arrived(m):
        wait_for(rows_of(m, 4 * 96), d_recv.at[m])

    def dispatch(h):
        for n in range(SEGS // 2):
            cut = slice(h * HALF + n * 256, h * HALF + (n + 1) * 256)
            spread(n, dot(picks, tok[:, cut], NN))
        narrow(send1.at[h])

    with scope("line"):
        line_here()
    with scope("load_wait"):
        for load in loads:
            load.wait()
    for m in range(3):
        own_along(m, 0)
    own_along(0, 1)
    with scope("tok_wait"):
        inputs[1].wait()
    with scope("dispatch0"):
        dispatch(0)
    with scope("plane"):
        plane_here()
    exchange(0, 0, send1, mid1.at[0, :, p], p, on_p)
    with scope("dispatch1"):
        dispatch(1)
    inputs[2].wait()
    exchange(0, 1, send1, mid1.at[1, :, p], p, on_p)
    for m in range(4):
        go(across(m, 0))
    with scope("router"):
        for h in range(HALVES):
            mid1[h, :, p] = send1[h, p]
        logits = dot(router[...], tok[...], NT)
        top = jnp.max(logits, axis=0, keepdims=True)
        log_total = top + jnp.log(jnp.sum(jnp.exp(logits - top), axis=0, keepdims=True))
        local_sum = jnp.sum(log_total * log_total, axis=1, keepdims=True)
        zs1[...] = jnp.broadcast_to(local_sum, zs1.shape)
        zg1[p] = jnp.broadcast_to(local_sum, zs1.shape)
        chosen0 = jnp.sum(jnp.where(hot0, logits, 0.0), axis=0, keepdims=True)
        chosen1 = jnp.sum(jnp.where(hot1, logits, 0.0), axis=0, keepdims=True)
        peak = jnp.maximum(chosen0, chosen1)
        exp0, exp1 = jnp.exp(chosen0 - peak), jnp.exp(chosen1 - peak)
        weight0, weight1 = exp0 / (exp0 + exp1), exp1 / (exp0 + exp1)
        mix = jnp.where(in0, weight0, jnp.where(in1, weight1, 0.0)).T
        mix_high[...] = mix.astype(jnp.bfloat16)
        mix_low[...] = (mix - mix.astype(jnp.bfloat16).astype(jnp.float32)).astype(jnp.bfloat16)
    z_exchange(0, zs1, zg1, p, on_p)
    with scope("p1_0"):
        landed(0, 0)
    with scope("relay_gu"):
        relay(0)
        relay(1)
    own_along(1, 1)
    with scope("p1_1s"):
        early_out(0, 1)
    exchange(1, 0, mid1, got1.at[0, q], q, on_q)
    with scope("relay_d0"):
        relay(2)
    own_along(2, 1)
    own_along(3, 0)
    own_along(3, 1)
    with scope("p1_1"):
        landed(0, 1)
    exchange(1, 1, mid1, got1.at[1, q], q, on_q)
    for h in range(HALVES):
        got1[h, q] = mid1[h, q]
    with scope("pass_g"):
        pass_neighbours(0)
        pass_far(0)
    z_landed(0)
    z_row = jnp.sum(zg1[...], axis=0)
    zs2[...] = z_row
    zg2[q] = z_row
    with scope("p2_0"):
        landed(1, 0)
    with scope("rows_0"):
        to_rows(got1, 0)
    z_exchange(1, zs2, zg2, q, on_q)
    with scope("far_u"):
        pass_far(1)

    def project(h, m, n):
        across_k = slice(h * HALF, (h + 1) * HALF)
        return dot(rows[:, across_k], gate_up[m, n * 256 : (n + 1) * 256, across_k], NT)

    def first_half(m):
        with scope("ffn_0%d" % m):
            for n in range(FF // 256):
                acc[m, :, n * 256 : (n + 1) * 256] = project(0, m, n)

    with scope("arrived_0"):
        arrived(0)
    first_half(0)
    with scope("pass_u"):
        pass_neighbours(1)
    with scope("arrived_1"):
        arrived(1)
    first_half(1)
    with scope("far_d0"):
        pass_far(2)
    with scope("p2_1"):
        landed(1, 1)
    with scope("pass_d0"):
        pass_neighbours(2)
    with scope("rows_1"):
        to_rows(got1, 1)
    with scope("ffn_1"):
        for n in range(FF // 256):
            cut = slice(n * 256, (n + 1) * 256)
            gated = acc[0, :, cut] + project(1, 0, n)
            upped = acc[1, :, cut] + project(1, 1, n)
            hidden[:, cut] = (gated / (1.0 + jnp.exp(-gated)) * upped).astype(jnp.bfloat16)
    for h in range(HALVES):
        with scope("far_d%d" % h):
            if h == 1:
                relay(3)
                pass_neighbours(3)
                pass_far(3)
        with scope("arrived_d%d" % h):
            arrived(2 + h)
        with scope("down_%d" % h):
            for n in range(SEGS // 2):
                spread(n, dot(hidden[...], downs[h, :, n * 256 : (n + 1) * 256], NN))
            narrow(send2.at[h])
        exchange(2, h, send2, mid2.at[h, :, q], q, on_q)
    z_landed(1)
    z_plane = jnp.sum(zg2[...], axis=0)
    zs3[...] = z_plane
    zg3[d] = z_plane
    for h in range(HALVES):
        mid2[h, :, q] = send2[h, q]
    z_exchange(2, zs3, zg3, d, at_dp)
    with scope("p3_0"):
        landed(2, 0)
    with scope("p3_1s"):
        early_out(2, 1)
    exchange(3, 0, mid2, got2.at[0, p], p, on_p)
    z_landed(2)
    total = jnp.sum(zg3[...], axis=0)
    z_val[...] = total[0:1, :] / jnp.float32(tokens_here * 512)
    z_store = pltpu.make_async_copy(z_val, z_out, load_sem.at[2])
    with scope("p3_1"):
        landed(2, 1)
    exchange(3, 1, mid2, got2.at[1, p], p, on_p)
    for h in range(HALVES):
        got2[h, p] = mid2[h, p]
    with scope("outs"):
        out_of(0, 0)
        late_out(0, 1)
        late_out(2, 1)
        out_of(1, 0)
        out_of(1, 1)
        out_of(2, 0)
        for phase in range(3):
            wait_for(zg1.at[pl.ds(0, RING - 1)], z_send.at[phase])
        for m in range(4):
            wait_for(rows_of(m, 6 * 48), x_send.at[m])
            wait_for(rows_of(m, 4 * 96), d_send.at[m])
    z_store.start()
    stores = [z_store]
    for h in range(HALVES):
        with scope("p4_%d" % h):
            landed(3, h)
        with scope("rows2_%d" % h):
            to_rows(got2, h)
        with scope("mix_%d" % h):
            for n in range(SEGS // 2):
                cut = slice(h * HALF + n * 256, h * HALF + (n + 1) * 256)
                part = rows[:, cut]
                mixed = dot(mix_high[...], part, NN) + dot(mix_low[...], part, NN)
                mixture[:, cut] = mixed.astype(jnp.bfloat16)
        cut = slice(h * HALF, (h + 1) * HALF)
        stores.append(pltpu.make_async_copy(mixture.at[:, cut], out.at[:, cut], load_sem.at[h]))
        stores[-1].start()
    with scope("end"):
        out_of(3, 0)
        out_of(3, 1)
        for store in stores:
            store.wait()


def on_device(tokens, router_weight, route_ids, gate_weight, up_weight, down_weight):
    rows_here, width = tokens.shape
    blocks = (HALVES, RING, RING, BLOCK, LANES)
    bf16, f32 = jnp.bfloat16, jnp.float32
    hbm = pl.BlockSpec(memory_space=pltpu.HBM)
    small = (8, LANES)
    dma = pltpu.SemaphoreType.DMA
    mixture, z_loss = pl.pallas_call(
        kernel,
        out_shape=(
            jax.ShapeDtypeStruct((rows_here, width), bf16),
            jax.ShapeDtypeStruct((1, LANES), f32),
        ),
        in_specs=[hbm] * 6,
        out_specs=(hbm, hbm),
        scratch_shapes=[
            pltpu.VMEM((rows_here, width), bf16),
            pltpu.VMEM(router_weight.shape[::-1], bf16),
            pltpu.VMEM(route_ids.shape[::-1], jnp.int32),
            pltpu.VMEM((SLOTS * SEGS, LANES), f32),
            pltpu.VMEM(blocks, bf16),
            pltpu.VMEM(blocks, bf16),
            pltpu.VMEM(blocks, bf16),
            pltpu.VMEM((SLOTS, width), bf16),
            pltpu.VMEM((2, SLOTS, FF), f32),
            pltpu.VMEM((SLOTS, FF), bf16),
            pltpu.VMEM(blocks, bf16),
            pltpu.VMEM(blocks, bf16),
            pltpu.VMEM(blocks, bf16),
            pltpu.VMEM((2, FF, width), bf16),
            pltpu.VMEM((HALVES, FF, HALF), bf16),
            pltpu.VMEM((rows_here, width), bf16),
            pltpu.VMEM((rows_here, SLOTS), bf16),
            pltpu.VMEM((rows_here, SLOTS), bf16),
            pltpu.VMEM((1, LANES), f32),
            pltpu.VMEM(small, f32),
            pltpu.VMEM(small, f32),
            pltpu.VMEM(small, f32),
            pltpu.VMEM((8,) + small, f32),
            pltpu.VMEM((8,) + small, f32),
            pltpu.VMEM((8,) + small, f32),
            dma((7,)),
            dma((4, HALVES, 2)),
            dma((4, HALVES)),
            dma((3,)),
            dma((3,)),
            dma((4,)),
            dma((2, 4, 3)),
            dma((4,)),
            dma((4,)),
            pltpu.SemaphoreType.REGULAR,
            pltpu.SemaphoreType.REGULAR,
        ],
        compiler_params=pltpu.CompilerParams(
            collective_id=0, has_side_effects=True, vmem_limit_bytes=60 * 1024 * 1024
        ),
    )(tokens, router_weight.T, route_ids.T, gate_weight, up_weight, down_weight)
    return mixture, z_loss[0, 0]


def solution(mesh):
    return jax.shard_map(
        on_device,
        mesh=mesh,
        in_specs=(
            P(BOTH, None),
            P(),
            P(BOTH, None),
            P("expert", "dp", None),
            P("expert", "dp", None),
            P("expert", "dp", None),
        ),
        out_specs=(P(BOTH, None), P()),
        check_vma=False,
    )
```

```python
import jax
import jax.numpy as jnp
from jax import lax
from jax.experimental import pallas as pl
from jax.experimental.pallas import tpu as pltpu
from jax.sharding import PartitionSpec as P

MESH = pl.DeviceIdType.MESH
BOTH = ("dp", "expert")
RING = 8
CAPACITY = 5
HALVES = 2
SEGS = 8
LANES = 128
HALF = SEGS * LANES
BLOCK = CAPACITY * SEGS
SLOTS = RING * RING * CAPACITY
FF = 768
NT = (((1,), (1,)), ((), ()))
NN = (((1,), (0,)), ((), ()))
OFFSETS = (3, 5, 4, 2, 6, 1, 7)
EARLY = OFFSETS[:5]
scope = jax.named_scope


def dot(a, b, dims):
    return lax.dot_general(a, b, dims, preferred_element_type=jnp.float32)


def kernel(
    tok_hbm,
    router_hbm,
    ids_hbm,
    gate,
    up,
    down,
    out0,
    out1,
    out2,
    out3,
    z_out,
    tok,
    router,
    ids,
    wide,
    send1,
    mid1,
    got1,
    rows,
    acc,
    hidden,
    send2,
    mid2,
    got2,
    gate_up,
    downs,
    mix_high,
    mix_low,
    z_val,
    zs1,
    zs2,
    zs3,
    zg1,
    zg2,
    zg3,
    load_sem,
    e_send,
    e_recv,
    z_send,
    z_recv,
    x_send,
    x_recv,
    d_send,
    d_recv,
    line,
    plane,
):
    outs = (out0, out1, out2, out3)
    d = lax.axis_index("dp")
    e = lax.axis_index("expert")
    x, c = d // 2, lax.rem(d, 2)
    z, y = e // RING, lax.rem(e, RING)
    p = y * (1 - c) + z * c
    q = z * (1 - c) + y * c

    def on_p(v):
        return {"dp": d, "expert": (z * RING + v) * (1 - c) + (v * RING + y) * c}

    def on_q(v):
        return {"dp": d, "expert": (v * RING + y) * (1 - c) + (z * RING + v) * c}

    def at_dp(v):
        return {"dp": v, "expert": e}

    def shard(x_at, c_at):
        return 2 * lax.rem(x_at, 4) + c_at

    own, left, right, far = (shard(x + k, c) for k in (0, 3, 1, 2))

    inputs = []
    for m, (src, dst) in enumerate(((ids_hbm, ids), (tok_hbm, tok), (router_hbm, router))):
        inputs.append(pltpu.make_async_copy(src, dst, load_sem.at[4 + m]))
        inputs[-1].start()

    barrier = pltpu.get_barrier_semaphore()
    other = at_dp(x * 2 + 1 - c)
    for k in OFFSETS:
        for peer in (z * RING + lax.rem(y + k, RING), lax.rem(z + k, RING) * RING + y):
            pl.semaphore_signal(
                barrier, 1, device_id={"dp": x * 2 + 1, "expert": peer}, device_id_type=MESH
            )
    for k in range(1, 4):
        pl.semaphore_signal(barrier, 1, device_id=at_dp(shard(x + k, 0)), device_id_type=MESH)

    @pl.when(c == 1)
    def _():
        pl.semaphore_signal(barrier, 1, device_id=other, device_id_type=MESH)

    def line_here():
        @pl.when(c == 0)
        def _():
            pl.semaphore_wait(barrier, 7)
            pl.semaphore_signal(line, 1, device_id=other, device_id_type=MESH)

        @pl.when(c == 1)
        def _():
            pl.semaphore_wait(line, 1)

    def plane_here():
        @pl.when(c == 1)
        def _():
            pl.semaphore_wait(barrier, 4 * (RING - 1))
            pl.semaphore_signal(plane, 1, device_id=other, device_id_type=MESH)

        @pl.when(c == 0)
        def _():
            pl.semaphore_wait(plane, 1)

    def piece(m, dev, first, count):
        part = pl.ds(pl.multiple_of(96 * dev + first, 16), count)
        return gate_up.at[m, part, :] if m < 2 else downs.at[m - 2, part, :]

    loads = []
    for m in range(4):
        src = (gate.at[0], up.at[0], down.at[0, :, 0:HALF], down.at[0, :, HALF:])[m]
        loads.append(pltpu.make_async_copy(src, piece(m, own, 0, 96), load_sem.at[m]))
        loads[-1].start()

    with scope("ids_wait"):
        inputs[0].wait()
    experts, tokens_here = router.shape[0], tok.shape[0]
    expert_at = lax.broadcasted_iota(jnp.int32, (experts, tokens_here), 0)
    id0, id1 = ids[0:1, :], ids[1:2, :]
    hot0, hot1 = id0 == expert_at, id1 == expert_at

    row_at = lax.broadcasted_iota(jnp.int32, (tokens_here, tokens_here), 0)
    col_at = lax.broadcasted_iota(jnp.int32, (tokens_here, tokens_here), 1)
    earlier = jnp.where(row_at < col_at, 1.0, 0.0).astype(jnp.bfloat16)
    one0 = jnp.where(hot0, 1.0, 0.0)
    one1 = jnp.where(hot1, 1.0, 0.0)
    before0 = dot(one0.astype(jnp.bfloat16), earlier, NN)
    before1 = dot(one1.astype(jnp.bfloat16), earlier, NN) + jnp.sum(one0, axis=1, keepdims=True)
    place0 = jnp.sum(before0 * one0, axis=0, keepdims=True).astype(jnp.int32)
    place1 = jnp.sum(before1 * one1, axis=0, keepdims=True).astype(jnp.int32)

    def ordinal(v):
        return jnp.where(c == 0, (v & 7) * RING + (v >> 3), v)

    slot0 = ordinal(id0) * CAPACITY + place0
    slot1 = ordinal(id1) * CAPACITY + place1
    slot_at = lax.broadcasted_iota(jnp.int32, (SLOTS, tokens_here), 0)
    in0, in1 = slot0 == slot_at, slot1 == slot_at
    picks = jnp.where(in0 | in1, 1.0, 0.0).astype(jnp.bfloat16)

    def narrow(dst):
        @pl.loop(0, RING)
        def _(a):
            for b in range(RING):
                start = pl.multiple_of((a * RING + b) * BLOCK, BLOCK)
                dst[a, b] = wide[pl.ds(start, BLOCK), :].astype(jnp.bfloat16)

    def spread(n, chunk):
        for i in range(2):
            wide[pl.ds(2 * n + i, SLOTS, stride=SEGS), :] = chunk[:, i * LANES : (i + 1) * LANES]

    def to_rows(src, h):
        @pl.loop(0, RING)
        def _(a):
            for b in range(RING):
                start = pl.multiple_of((a * RING + b) * BLOCK, BLOCK)
                wide[pl.ds(start, BLOCK), :] = src[h, a, b].astype(jnp.float32)

        for j in range(SEGS):
            part = wide[pl.ds(j, SLOTS, stride=SEGS), :]
            cut = slice(h * HALF + j * LANES, h * HALF + (j + 1) * LANES)
            rows[:, cut] = part.astype(jnp.bfloat16)

    def exchange(phase, h, src, dst, me, peer):
        for k in OFFSETS:
            v = lax.rem(me + k, RING)
            pltpu.make_async_remote_copy(
                src.at[h, v],
                dst,
                e_send.at[phase, h, 0 if k in EARLY else 1],
                e_recv.at[phase, h],
                device_id=peer(v),
                device_id_type=MESH,
            ).start()

    def wait_for(ref, sem):
        pltpu.make_async_copy(ref, ref, sem).wait()

    def landed(phase, h):
        wait_for(send1.at[h, pl.ds(0, RING - 1)], e_recv.at[phase, h])

    def early_out(phase, h):
        wait_for(send1.at[h, pl.ds(0, len(EARLY))], e_send.at[phase, h, 0])

    def late_out(phase, h):
        if len(EARLY) == RING - 1:
            return
        wait_for(send1.at[h, pl.ds(0, RING - 1 - len(EARLY))], e_send.at[phase, h, 1])

    def out_of(phase, h):
        early_out(phase, h)
        late_out(phase, h)

    def z_exchange(phase, src, dst, me, peer):
        for k in range(1, RING):
            v = lax.rem(me + k, RING)
            pltpu.make_async_remote_copy(
                src,
                dst.at[me],
                z_send.at[phase],
                z_recv.at[phase],
                device_id=peer(v),
                device_id_type=MESH,
            ).start()

    def z_landed(phase):
        wait_for(zg1.at[pl.ds(0, RING - 1)], z_recv.at[phase])

    def along(m, go_right, stage):
        if go_right:
            dev, first = (own, 0) if stage == 0 else (own, 48) if stage == 1 else (left, 0)
        else:
            dev, first = (own, 48) if stage == 0 else (own, 0) if stage == 1 else (right, 48)
        side = 0 if go_right else 1
        return pltpu.make_async_remote_copy(
            piece(m, dev, first, 48),
            piece(m, dev, first, 48),
            x_send.at[m],
            x_recv.at[side, m, stage],
            device_id=at_dp(right if go_right else left),
            device_id_type=MESH,
        )

    def across(m, which):
        dev = (own, left, right, far)[which]
        return pltpu.make_async_remote_copy(
            piece(m, dev, 0, 96),
            piece(m, dev, 0, 96),
            d_send.at[m],
            d_recv.at[m],
            device_id=at_dp(x * 2 + 1 - c),
            device_id_type=MESH,
        )

    def go(copy):
        copy.start()

    def own_along(m, stage):
        go(along(m, True, stage))
        go(along(m, False, stage))

    def relay(m):
        along(m, True, 0).wait_recv()
        go(along(m, True, 2))
        along(m, False, 0).wait_recv()
        go(along(m, False, 2))

    def pass_neighbours(m):
        along(m, True, 1).wait_recv()
        go(across(m, 1))
        along(m, False, 1).wait_recv()
        go(across(m, 2))

    def pass_far(m):
        along(m, True, 2).wait_recv()
        along(m, False, 2).wait_recv()
        go(across(m, 3))

    def rows_of(m, count):
        return gate_up.at[m, pl.ds(0, count)] if m < 2 else downs.at[m - 2, pl.ds(0, count)]

    def arrived(m):
        wait_for(rows_of(m, 4 * 96), d_recv.at[m])

    def dispatch(h):
        for n in range(SEGS // 2):
            cut = slice(h * HALF + n * 256, h * HALF + (n + 1) * 256)
            spread(n, dot(picks, tok[:, cut], NN))
        narrow(send1.at[h])

    with scope("line"):
        line_here()
    with scope("load_wait"):
        for load in loads:
            load.wait()
    for m in range(3):
        own_along(m, 0)
    own_along(0, 1)
    with scope("tok_wait"):
        inputs[1].wait()
    with scope("dispatch0"):
        dispatch(0)
    with scope("plane"):
        plane_here()
    exchange(0, 0, send1, mid1.at[0, :, p], p, on_p)
    with scope("dispatch1"):
        dispatch(1)
    inputs[2].wait()
    exchange(0, 1, send1, mid1.at[1, :, p], p, on_p)
    for m in range(4):
        go(across(m, 0))
    with scope("router"):
        for h in range(HALVES):
            mid1[h, :, p] = send1[h, p]
        logits = dot(router[...], tok[...], NT)
        top = jnp.max(logits, axis=0, keepdims=True)
        log_total = top + jnp.log(jnp.sum(jnp.exp(logits - top), axis=0, keepdims=True))
        local_sum = jnp.sum(log_total * log_total, axis=1, keepdims=True)
        zs1[...] = jnp.broadcast_to(local_sum, zs1.shape)
        zg1[p] = jnp.broadcast_to(local_sum, zs1.shape)
        chosen0 = jnp.sum(jnp.where(hot0, logits, 0.0), axis=0, keepdims=True)
        chosen1 = jnp.sum(jnp.where(hot1, logits, 0.0), axis=0, keepdims=True)
        peak = jnp.maximum(chosen0, chosen1)
        exp0, exp1 = jnp.exp(chosen0 - peak), jnp.exp(chosen1 - peak)
        weight0, weight1 = exp0 / (exp0 + exp1), exp1 / (exp0 + exp1)
        mix = jnp.where(in0, weight0, jnp.where(in1, weight1, 0.0)).T
        mix_high[...] = mix.astype(jnp.bfloat16)
        mix_low[...] = (mix - mix.astype(jnp.bfloat16).astype(jnp.float32)).astype(jnp.bfloat16)
    z_exchange(0, zs1, zg1, p, on_p)
    with scope("p1_0"):
        landed(0, 0)
    with scope("relay_gu"):
        relay(0)
        relay(1)
    own_along(1, 1)
    with scope("p1_1s"):
        early_out(0, 1)
    exchange(1, 0, mid1, got1.at[0, q], q, on_q)
    with scope("relay_d0"):
        relay(2)
    own_along(2, 1)
    own_along(3, 0)
    own_along(3, 1)
    with scope("p1_1"):
        landed(0, 1)
    exchange(1, 1, mid1, got1.at[1, q], q, on_q)
    for h in range(HALVES):
        got1[h, q] = mid1[h, q]
    with scope("pass_g"):
        pass_neighbours(0)
        pass_far(0)
    z_landed(0)
    z_row = jnp.sum(zg1[...], axis=0)
    zs2[...] = z_row
    zg2[q] = z_row
    with scope("p2_0"):
        landed(1, 0)
    with scope("rows_0"):
        to_rows(got1, 0)
    z_exchange(1, zs2, zg2, q, on_q)
    with scope("far_u"):
        pass_far(1)

    def project(h, m, n):
        across_k = slice(h * HALF, (h + 1) * HALF)
        return dot(rows[:, across_k], gate_up[m, n * 256 : (n + 1) * 256, across_k], NT)

    def first_half(m):
        with scope("ffn_0%d" % m):
            for n in range(FF // 256):
                acc[m, :, n * 256 : (n + 1) * 256] = project(0, m, n)

    with scope("arrived_0"):
        arrived(0)
    first_half(0)
    with scope("pass_u"):
        pass_neighbours(1)
    with scope("arrived_1"):
        arrived(1)
    first_half(1)
    with scope("far_d0"):
        pass_far(2)
    with scope("p2_1"):
        landed(1, 1)
    with scope("pass_d0"):
        pass_neighbours(2)
    with scope("rows_1"):
        to_rows(got1, 1)
    with scope("ffn_1"):
        for n in range(FF // 256):
            cut = slice(n * 256, (n + 1) * 256)
            gated = acc[0, :, cut] + project(1, 0, n)
            upped = acc[1, :, cut] + project(1, 1, n)
            hidden[:, cut] = (gated / (1.0 + jnp.exp(-gated)) * upped).astype(jnp.bfloat16)
    for h in range(HALVES):
        with scope("far_d%d" % h):
            if h == 1:
                relay(3)
                pass_neighbours(3)
                pass_far(3)
        with scope("arrived_d%d" % h):
            arrived(2 + h)
        with scope("down_%d" % h):
            for n in range(SEGS // 2):
                spread(n, dot(hidden[...], downs[h, :, n * 256 : (n + 1) * 256], NN))
            narrow(send2.at[h])
        exchange(2, h, send2, mid2.at[h, :, q], q, on_q)
    z_landed(1)
    z_plane = jnp.sum(zg2[...], axis=0)
    zs3[...] = z_plane
    zg3[d] = z_plane
    for h in range(HALVES):
        mid2[h, :, q] = send2[h, q]
    z_exchange(2, zs3, zg3, d, at_dp)
    with scope("p3_0"):
        landed(2, 0)
    with scope("p3_1s"):
        early_out(2, 1)
    exchange(3, 0, mid2, got2.at[0, p], p, on_p)
    z_landed(2)
    total = jnp.sum(zg3[...], axis=0)
    z_val[...] = total[0:1, :] / jnp.float32(tokens_here * 512)
    z_store = pltpu.make_async_copy(z_val, z_out, load_sem.at[2])
    with scope("p3_1"):
        landed(2, 1)
    exchange(3, 1, mid2, got2.at[1, p], p, on_p)
    for h in range(HALVES):
        got2[h, p] = mid2[h, p]
    with scope("outs"):
        out_of(0, 0)
        late_out(0, 1)
        late_out(2, 1)
        out_of(1, 0)
        out_of(1, 1)
        out_of(2, 0)
        for phase in range(3):
            wait_for(zg1.at[pl.ds(0, RING - 1)], z_send.at[phase])
        for m in range(4):
            wait_for(rows_of(m, 6 * 48), x_send.at[m])
            wait_for(rows_of(m, 4 * 96), d_send.at[m])
    z_store.start()
    stores = [z_store]
    for h in range(HALVES):
        with scope("p4_%d" % h):
            landed(3, h)
        with scope("rows2_%d" % h):
            to_rows(got2, h)
        with scope("mix_%d" % h):
            for n in range(SEGS // 2):
                cut = slice(h * HALF + n * 256, h * HALF + (n + 1) * 256)
                part = rows[:, cut]
                mixed = dot(mix_high[...], part, NN) + dot(mix_low[...], part, NN)
                piece_at, first = divmod(h * HALF + n * 256, 512)
                outs[piece_at][:, first : first + 256] = mixed.astype(jnp.bfloat16)
    with scope("end"):
        out_of(3, 0)
        out_of(3, 1)
        for store in stores:
            store.wait()


def on_device(tokens, router_weight, route_ids, gate_weight, up_weight, down_weight):
    rows_here, width = tokens.shape
    blocks = (HALVES, RING, RING, BLOCK, LANES)
    bf16, f32 = jnp.bfloat16, jnp.float32
    vmem = pl.BlockSpec(memory_space=pltpu.VMEM)
    hbm = pl.BlockSpec(memory_space=pltpu.HBM)
    small = (8, LANES)
    dma = pltpu.SemaphoreType.DMA
    *pieces, z_loss = pl.pallas_call(
        kernel,
        out_shape=(
            *[jax.ShapeDtypeStruct((rows_here, width // 4), bf16)] * 4,
            jax.ShapeDtypeStruct((1, LANES), f32),
        ),
        in_specs=[hbm] * 6,
        out_specs=(*[vmem] * 4, hbm),
        scratch_shapes=[
            pltpu.VMEM((rows_here, width), bf16),
            pltpu.VMEM(router_weight.shape[::-1], bf16),
            pltpu.VMEM(route_ids.shape[::-1], jnp.int32),
            pltpu.VMEM((SLOTS * SEGS, LANES), f32),
            pltpu.VMEM(blocks, bf16),
            pltpu.VMEM(blocks, bf16),
            pltpu.VMEM(blocks, bf16),
            pltpu.VMEM((SLOTS, width), bf16),
            pltpu.VMEM((2, SLOTS, FF), f32),
            pltpu.VMEM((SLOTS, FF), bf16),
            pltpu.VMEM(blocks, bf16),
            pltpu.VMEM(blocks, bf16),
            pltpu.VMEM(blocks, bf16),
            pltpu.VMEM((2, FF, width), bf16),
            pltpu.VMEM((HALVES, FF, HALF), bf16),
            pltpu.VMEM((rows_here, SLOTS), bf16),
            pltpu.VMEM((rows_here, SLOTS), bf16),
            pltpu.VMEM((1, LANES), f32),
            pltpu.VMEM(small, f32),
            pltpu.VMEM(small, f32),
            pltpu.VMEM(small, f32),
            pltpu.VMEM((8,) + small, f32),
            pltpu.VMEM((8,) + small, f32),
            pltpu.VMEM((8,) + small, f32),
            dma((7,)),
            dma((4, HALVES, 2)),
            dma((4, HALVES)),
            dma((3,)),
            dma((3,)),
            dma((4,)),
            dma((2, 4, 3)),
            dma((4,)),
            dma((4,)),
            pltpu.SemaphoreType.REGULAR,
            pltpu.SemaphoreType.REGULAR,
        ],
        compiler_params=pltpu.CompilerParams(
            collective_id=0, has_side_effects=True, vmem_limit_bytes=55889100
        ),
    )(tokens, router_weight.T, route_ids.T, gate_weight, up_weight, down_weight)
    return jnp.concatenate(pieces, axis=1), z_loss[0, 0]


def solution(mesh):
    return jax.shard_map(
        on_device,
        mesh=mesh,
        in_specs=(
            P(BOTH, None),
            P(),
            P(BOTH, None),
            P("expert", "dp", None),
            P("expert", "dp", None),
            P("expert", "dp", None),
        ),
        out_specs=(P(BOTH, None), P()),
        check_vma=False,
    )
```
